32 devices in a mesh: rep: 4 (over x, y), dp: 8 (over z, core).
Axes of the slice: x: 2, y: 2, z: 4, core: 2. Of those that a mesh axis runs over, the one named last changes fastest.
Arguments:
- x: bfloat16 [32, 2048, 640], P(('rep', 'dp')), parts along dimension 0
- dy: bfloat16 [32, 2048, 640], P(('rep', 'dp')), parts along dimension 0
- w_gate: bfloat16 [2, 640, 2560], replicated
- w_up: bfloat16 [2, 640, 2560], replicated
- w_down: bfloat16 [2, 2560, 640], replicated
- m_w_gate: float32 [2, 640, 2560], replicated
- m_w_up: float32 [2, 640, 2560], replicated
- m_w_down: float32 [2, 2560, 640], replicated
- v_w_gate: float32 [2, 640, 2560], replicated
- v_w_up: float32 [2, 640, 2560], replicated
- v_w_down: float32 [2, 2560, 640], replicated
Outputs:
- output 1: bfloat16 [8, 640, 2560], P('rep'), parts along dimension 0
- output 2: bfloat16 [8, 640, 2560], P('rep'), parts along dimension 0
- output 3: bfloat16 [8, 2560, 640], P('rep'), parts along dimension 0
- output 4: float32 [8, 640, 2560], P('rep'), parts along dimension 0
- output 5: float32 [8, 640, 2560], P('rep'), parts along dimension 0
- output 6: float32 [8, 2560, 640], P('rep'), parts along dimension 0
- output 7: float32 [8, 640, 2560], P('rep'), parts along dimension 0
- output 8: float32 [8, 640, 2560], P('rep'), parts along dimension 0
- output 9: float32 [8, 2560, 640], P('rep'), parts along dimension 0
There are 4 independent parts. The reference program is written for one: setup_inputs(seed, part) draws one part's arguments, and reference() takes and returns one part's arrays. A program takes and returns all parts, laid end to end along the dimension named above; an argument that names none is the same for every part.
All inputs are finite; a program needn't handle non-finite values.
Results may differ from the reference program's by a relative error of at most 0.022.
Values are sent between devices in bfloat16 or wider.
A program may use at most 2.5 GiB of HBM per device.

```python
import jax
import jax.numpy as jnp
from jax import lax

SEQUENCES = 8
TOKENS = 2048
D = 640
FF = 2560
LAYERS = 2
NAMES = ("w_gate", "w_up", "w_down")
SHAPES = {"w_gate": (LAYERS, D, FF), "w_up": (LAYERS, D, FF), "w_down": (LAYERS, FF, D)}


def bump(key, n, height):
    away = (jnp.arange(n, dtype=jnp.int32) - jax.random.randint(key, (), 0, n, jnp.int32)) % n
    return jnp.where(away < n // 8, height, 1.0)


def together(key, own, strength):
    shared = jax.random.normal(key, own.shape[1:], jnp.float32)
    return (own + strength * shared) * lax.rsqrt(1 + strength * strength)


def setup_inputs(seed: int = 0, part: int = 0) -> dict:
    kx, kdy, ka, kb, kz, kf, kh, kl, *keys = jax.random.split(jax.random.key(seed), 8 + 3 * len(NAMES))
    kx, kdy, ka, kb = (jax.random.fold_in(k, part) for k in (kx, kdy, ka, kb))
    kw, km, kv = (keys[i::3] for i in range(3))
    shape = (SEQUENCES, TOKENS, D)
    much_x, much_dy = jax.random.uniform(kz, (2,), jnp.float32, 0.0, 1.0)
    loud = 2.0 ** jax.random.uniform(jax.random.fold_in(kz, 1), (), jnp.float32, -1.0, 2.0)
    layers = 2.0 ** jax.random.uniform(kl, (LAYERS, 1, 1), jnp.float32, -1.0, 1.0)
    x = together(ka, jax.random.normal(kx, shape, jnp.float32), much_x) * bump(kf, D, 4.0)
    dy = together(kb, jax.random.normal(kdy, shape, jnp.float32), much_dy)
    drawn = {"x": x.astype(jnp.bfloat16), "dy": (loud * dy * (SEQUENCES * TOKENS) ** -0.5).astype(jnp.bfloat16)}
    for key, name in zip(kw, NAMES, strict=True):
        w = jax.random.normal(key, SHAPES[name], jnp.float32) * SHAPES[name][1] ** -0.5
        drawn[name] = (w * {"w_gate": 1.0, "w_up": bump(kh, FF, 4.0), "w_down": layers}[name]).astype(jnp.bfloat16)
    for key, name in zip(km, NAMES, strict=True):
        drawn[f"m_{name}"] = 0.1 * jax.random.normal(key, SHAPES[name], jnp.float32)
    for key, name in zip(kv, NAMES, strict=True):
        drawn[f"v_{name}"] = jax.random.uniform(key, SHAPES[name], jnp.float32, 0.005, 0.015)
    return drawn


def matmul(a, w):
    return jnp.dot(a, w, preferred_element_type=jnp.float32).astype(jnp.bfloat16)


def normed(h):
    wide = h.astype(jnp.float32)
    scale = lax.rsqrt(jnp.mean(wide**2, -1, keepdims=True) + 1e-6)
    return (wide * scale).astype(jnp.bfloat16)


def layer(h, w):
    a = normed(h)
    gate = jnp.dot(a, w["w_gate"], preferred_element_type=jnp.float32)
    up = jnp.dot(a, w["w_up"], preferred_element_type=jnp.float32)
    return h + matmul((jax.nn.silu(gate) * up).astype(jnp.bfloat16), w["w_down"])


def adamw(w, m, v, g):
    m = 0.9 * m + 0.1 * g
    v = 0.95 * v + 0.05 * g * g
    step = m * lax.rsqrt(v + 1e-8) + 0.1 * w
    return (w - 0.02 * step).astype(jnp.bfloat16), m, v


def clipped(gradients, sum_of_squares, count):
    factor = jnp.minimum(1.0, 0.5 * lax.rsqrt(sum_of_squares / count + 1e-30))
    return [g * factor for g in gradients]


def stack(weights, h):
    return lax.scan(lambda h, w: (layer(h, w), None), h, weights)[0]


def reference(x, dy, w_gate, w_up, w_down, m_w_gate, m_w_up, m_w_down, v_w_gate, v_w_up, v_w_down):
    weights = dict(zip(NAMES, (w_gate, w_up, w_down), strict=True))

    def take(so_far, sequence):
        h, by_y = sequence
        _, back = jax.vjp(lambda w: stack(w, h), weights)
        return jax.tree.map(lambda total, term: total + term.astype(jnp.float32), so_far, back(by_y)[0]), None

    none_yet = {name: jnp.zeros(w.shape, jnp.float32) for name, w in weights.items()}
    by_weights, _ = lax.scan(take, none_yet, (x, dy))
    gradients = [by_weights[name].astype(jnp.bfloat16).astype(jnp.float32) for name in NAMES]
    gradients = clipped(gradients, sum(jnp.sum(g * g) for g in gradients), sum(g.size for g in gradients))
    new = [
        adamw(w.astype(jnp.float32), m, v, g)
        for w, m, v, g in zip((w_gate, w_up, w_down), (m_w_gate, m_w_up, m_w_down), (v_w_gate, v_w_up, v_w_down), gradients, strict=True)
    ]
    return tuple(one[which] for which in range(3) for one in new)
```

```python
import functools

import jax
import jax.numpy as jnp
from jax import lax
from jax.experimental import pallas as pl
from jax.experimental.pallas import tpu as pltpu
from jax.sharding import PartitionSpec as P

NAMES = ("w_gate", "w_up", "w_down")
BLOCK = 256
F32, BF16 = jnp.float32, jnp.bfloat16
NT = (((1,), (1,)), ((), ()))


def dot(a, b):
    return jnp.dot(a, b, preferred_element_type=F32)


def dot_nt(a, b):
    return lax.dot_general(a, b, NT, preferred_element_type=F32)


def scale_of(wide):
    return lax.rsqrt(jnp.mean(wide * wide, -1, keepdims=True) + 1e-6)


def forward_kernel(tile, chunk, x, wg, wu, wd, out, wgb, wub, wdb, act, sems):
    tokens, ff = x.shape[0], wd.shape[1]
    chunks = ff // chunk

    def copies(f):
        part = pl.ds(pl.multiple_of(f * chunk, chunk), chunk)
        return (
            pltpu.make_async_copy(wg.at[0, :, part], wgb.at[:, part], sems.at[0, f]),
            pltpu.make_async_copy(wu.at[0, :, part], wub.at[:, part], sems.at[1, f]),
            pltpu.make_async_copy(wd.at[0, part, :], wdb.at[part, :], sems.at[2, f]),
        )

    for f in range(chunks):
        for copy in copies(f):
            copy.start()

    def rows_of(t, _):
        rows = pl.ds(pl.multiple_of(t * tile, tile), tile)
        wide = x[rows, :].astype(F32)
        a = (wide * scale_of(wide)).astype(BF16)

        def hidden(f, _):
            @pl.when(t == 0)
            def _():
                for copy in copies(f):
                    copy.wait()

            part = pl.ds(pl.multiple_of(f * chunk, chunk), chunk)
            gate = dot(a, wgb[:, part])
            up = dot(a, wub[:, part])
            act[:, part] = (gate * jax.nn.sigmoid(gate) * up).astype(BF16)
            return 0

        lax.fori_loop(0, chunks, hidden, 0)
        out[rows, :] = x[rows, :] + dot(act[...], wdb[...]).astype(BF16)
        return 0

    lax.fori_loop(0, tokens // tile, rows_of, 0)


def backward_kernel(
    tile, x, h, dy, wg, wu, wd, og, ou, od, squares,
    xbuf, hbuf, abuf, at, dbuf, dt, acc, wgu, wdb, act, dgu, grad, pair, edge, middle, final, turned,
    in_sem, w_sem, p_s, p_r, e_s, e_r, m_s, m_r, f_s, f_r, a_s, a_r, b_s, b_r, q_s, q_r, out_sem,
):
    tokens, d = abuf.shape
    blocks = wg.shape[2] // BLOCK
    total = 2 * blocks
    half, quarter = 3 * d // 2, 3 * d // 4
    place = lax.axis_index("dp")
    z, core = place // 2, place % 2
    is_middle = jnp.logical_and(z > 0, z < 3)
    is_edge = jnp.logical_not(is_middle)
    partner = z * 2 + 1 - core
    near = (z + 1 - 2 * (z % 2)) * 2 + core
    across = (3 - z) * 2 + core
    side = z // 2
    own, other = pl.multiple_of(core * half, half), pl.multiple_of((1 - core) * half, half)
    home = pl.multiple_of(own + side * quarter, quarter)
    away = pl.multiple_of(own + (1 - side) * quarter, quarter)

    def signal(barrier, device):
        pl.semaphore_signal(barrier, inc=1, device_id={"dp": device}, device_id_type=pl.DeviceIdType.MESH)

    barrier = pltpu.get_barrier_semaphore()
    signal(barrier, partner)
    signal(barrier, near)

    @pl.when(is_middle)
    def _():
        signal(barrier, across)

    pl.semaphore_wait(barrier, jnp.where(is_middle, 3, 2))

    def remote(src, dst, send, recv, device):
        return pltpu.make_async_remote_copy(
            src_ref=src, dst_ref=dst, send_sem=send, recv_sem=recv, device_id={"dp": device}, device_id_type=pl.DeviceIdType.MESH
        )

    def pair_copy(j):
        return remote(grad.at[j, pl.ds(other, half), :], pair.at[j], p_s.at[j], p_r.at[j], partner)

    def edge_copy(j):
        return remote(grad.at[j, pl.ds(own, half), :], edge.at[j], e_s.at[j], e_r.at[j], near)

    def middle_copy(j):
        return remote(grad.at[j, pl.ds(away, quarter), :], middle.at[j], m_s.at[j], m_r.at[j], across)

    def cross_copy(j, rows):
        return remote(final.at[j, pl.ds(rows, quarter), :], final.at[j, pl.ds(rows, quarter), :], f_s.at[j], f_r.at[j], across)

    def back_home(j):
        return remote(final.at[j, pl.ds(home, quarter), :], final.at[j, pl.ds(home, quarter), :], a_s.at[j], a_r.at[j], near)

    def back_away(j):
        return remote(final.at[j, pl.ds(away, quarter), :], final.at[j, pl.ds(away, quarter), :], b_s.at[j], b_r.at[j], near)

    def share_copy(j, rows):
        return remote(final.at[j, pl.ds(rows, half), :], final.at[j, pl.ds(rows, half), :], q_s.at[j], q_r.at[j], partner)

    def weight_copies(i):
        layer, j, slot = jnp.where(i < blocks, 1, 0), i % blocks, i % 2
        part = pl.ds(pl.multiple_of(j * BLOCK, BLOCK), BLOCK)
        return (
            pltpu.make_async_copy(wg.at[layer, :, part], wgu.at[slot, :, pl.ds(0, BLOCK)], w_sem.at[slot, 0]),
            pltpu.make_async_copy(wu.at[layer, :, part], wgu.at[slot, :, pl.ds(BLOCK, BLOCK)], w_sem.at[slot, 1]),
            pltpu.make_async_copy(wd.at[layer, part, :], wdb.at[slot], w_sem.at[slot, 2]),
        )

    def out_copies(k):
        layer, j, slot = jnp.where(k < blocks, 1, 0), k % blocks, k % 2
        part = pl.ds(pl.multiple_of(j * BLOCK, BLOCK), BLOCK)
        return (
            pltpu.make_async_copy(final.at[j, pl.ds(0, d), :], og.at[layer, :, part], out_sem.at[slot, 0]),
            pltpu.make_async_copy(final.at[j, pl.ds(d, d), :], ou.at[layer, :, part], out_sem.at[slot, 1]),
            pltpu.make_async_copy(turned.at[slot], od.at[layer, part, :], out_sem.at[slot, 2]),
        )

    inputs = (
        pltpu.make_async_copy(h, hbuf, in_sem.at[0]),
        pltpu.make_async_copy(dy, dbuf, in_sem.at[1]),
        pltpu.make_async_copy(x, xbuf, in_sem.at[2]),
    )
    for copy in inputs:
        copy.start()
    for copy in weight_copies(0):
        copy.start()
    squares[...] = jnp.zeros_like(squares)
    for copy in inputs:
        copy.wait()

    def tiles(body):
        def one(t, _):
            body(pl.ds(pl.multiple_of(t * tile, tile), tile))
            return 0

        lax.fori_loop(0, tokens // tile, one, 0)

    def norm_into(source, rows):
        wide = source[rows, :].astype(F32)
        a = (wide * scale_of(wide)).astype(BF16)
        abuf[rows, :] = a
        at[:, rows] = a.T

    def first(rows):
        norm_into(hbuf, rows)
        dt[:, rows] = dbuf[rows, :].T
        acc[rows, :] = jnp.zeros((tile, d), F32)

    tiles(first)

    def turn(rows):
        wide = hbuf[rows, :].astype(F32)
        by_a = acc[rows, :].astype(BF16).astype(F32)
        r = scale_of(wide)
        by_wide = by_a * r - wide * (r * r * r * jnp.mean(by_a * wide, -1, keepdims=True))
        by_h = by_wide.astype(BF16) + dbuf[rows, :]
        dbuf[rows, :] = by_h
        dt[:, rows] = by_h.T
        norm_into(xbuf, rows)

    def compute(i):
        j, slot = i % blocks, i % 2
        for copy in weight_copies(i):
            copy.wait()

        @pl.when(i + 1 < total)
        def _():
            for copy in weight_copies(i + 1):
                copy.start()

        @pl.when(i == blocks)
        def _():
            tiles(turn)

        def hidden(rows):
            gu = dot(abuf[rows, :], wgu[slot])
            by_act = dot_nt(dbuf[rows, :], wdb[slot]).astype(BF16).astype(F32)
            gate, up = gu[:, :BLOCK], gu[:, BLOCK:]
            s = jax.nn.sigmoid(gate)
            silu = gate * s
            act[rows, :] = (silu * up).astype(BF16)
            dgu[rows, :BLOCK] = (by_act * up * (s + silu * (1 - s))).astype(BF16)
            dgu[rows, BLOCK:] = (by_act * silu).astype(BF16)

        tiles(hidden)

        down = dot(dt[...], act[...]).astype(BF16)
        both = dot(at[...], dgu[...])
        grad[j, 2 * d :, :] = down
        grad[j, :d, :] = both[:, :BLOCK].astype(BF16)
        grad[j, d : 2 * d, :] = both[:, BLOCK:].astype(BF16)
        pair_copy(j).start()

        @pl.when(i < blocks)
        def _():
            def into(rows):
                acc[rows, :] += dot_nt(dgu[rows, :], wgu[slot])

            tiles(into)

    def wide(ref, j, rows, count):
        return ref[j, pl.ds(rows, count), :].astype(F32)

    def paired(k):
        j = k % blocks
        pair_copy(j).wait_recv()
        pair_copy(j).wait_send()

        @pl.when(is_edge)
        def _():
            grad[j, pl.ds(own, half), :] = (wide(grad, j, own, half) + wide(pair, j, 0, half)).astype(BF16)
            edge_copy(j).start()

    def so_far(j, rows):
        inside = pl.multiple_of(rows - own, quarter)
        return wide(grad, j, rows, quarter) + wide(pair, j, inside, quarter) + wide(edge, j, inside, quarter)

    def sides(k):
        j = k % blocks

        @pl.when(is_middle)
        def _():
            edge_copy(j).wait_recv()
            grad[j, pl.ds(away, quarter), :] = so_far(j, away).astype(BF16)
            middle_copy(j).start()

    def finished(k):
        j = k % blocks

        @pl.when(is_middle)
        def _():
            middle_copy(j).wait_recv()
            middle_copy(j).wait_send()
            final[j, pl.ds(home, quarter), :] = (so_far(j, home) + wide(middle, j, 0, quarter)).astype(BF16)
            cross_copy(j, home).start()
            back_home(j).start()

    def crossed(k):
        j = k % blocks

        @pl.when(is_middle)
        def _():
            cross_copy(j, away).wait_recv()
            cross_copy(j, home).wait_send()
            back_away(j).start()
            share_copy(j, own).start()

    def returned(k):
        j = k % blocks

        @pl.when(is_middle)
        def _():
            back_home(j).wait_send()
            back_away(j).wait_send()

        @pl.when(is_edge)
        def _():
            edge_copy(j).wait_send()
            back_home(j).wait_recv()
            back_away(j).wait_recv()
            share_copy(j, own).start()

    def shared(k):
        j = k % blocks
        share_copy(j, other).wait_recv()
        share_copy(j, own).wait_send()
        turned[k % 2] = final[j, 2 * d :, :].T
        for copy in out_copies(k):
            copy.start()
        for part in range(3):
            g = final[j, part * d : (part + 1) * d, :].astype(F32)
            squares[...] += jnp.sum((g * g).reshape(d // 8, 8, BLOCK), axis=0)

    def written(k):
        for copy in out_copies(k):
            copy.wait()

    stages = ((1, paired), (3, sides), (4, finished), (5, crossed), (7, returned), (8, shared), (9, written))

    def step(i, _):
        @pl.when(i < total)
        def _():
            compute(i)

        for lag, stage in stages:

            @pl.when(jnp.logical_and(i >= lag, i < total + lag))
            def _(lag=lag, stage=stage):
                stage(i - lag)

        return 0

    lax.fori_loop(0, total + stages[-1][0], step, 0)


def forward(x, weights, tile=512, chunk=512):
    tokens, d = x.shape
    ff = weights[0].shape[2]
    any_space = pl.BlockSpec(memory_space=pl.ANY)
    return pl.pallas_call(
        functools.partial(forward_kernel, min(tile, tokens), chunk),
        out_shape=jax.ShapeDtypeStruct(x.shape, BF16),
        in_specs=[pl.BlockSpec(memory_space=pltpu.VMEM)] + [any_space] * 3,
        out_specs=pl.BlockSpec(memory_space=pltpu.VMEM),
        scratch_shapes=[
            pltpu.VMEM((d, ff), BF16),
            pltpu.VMEM((d, ff), BF16),
            pltpu.VMEM((ff, d), BF16),
            pltpu.VMEM((min(tile, tokens), ff), BF16),
            pltpu.SemaphoreType.DMA((3, ff // chunk)),
        ],
        compiler_params=pltpu.CompilerParams(vmem_limit_bytes=48 * 2**20),
        name="forward",
    )(x, *weights)


def summed_gradients(x, h, dy, weights, tile=512):
    tokens, d = x.shape
    ff = weights[0].shape[2]
    blocks = ff // BLOCK
    tile = min(tile, tokens)
    any_space = pl.BlockSpec(memory_space=pl.ANY)
    dma = pltpu.SemaphoreType.DMA
    return pl.pallas_call(
        functools.partial(backward_kernel, tile),
        out_shape=[jax.ShapeDtypeStruct(w.shape, BF16) for w in weights] + [jax.ShapeDtypeStruct((8, BLOCK), F32)],
        in_specs=[any_space] * 6,
        out_specs=[any_space] * 3 + [pl.BlockSpec(memory_space=pltpu.VMEM)],
        scratch_shapes=[
            pltpu.VMEM((tokens, d), BF16),
            pltpu.VMEM((tokens, d), BF16),
            pltpu.VMEM((tokens, d), BF16),
            pltpu.VMEM((d, tokens), BF16),
            pltpu.VMEM((tokens, d), BF16),
            pltpu.VMEM((d, tokens), BF16),
            pltpu.VMEM((tokens, d), F32),
            pltpu.VMEM((2, d, 2 * BLOCK), BF16),
            pltpu.VMEM((2, BLOCK, d), BF16),
            pltpu.VMEM((tokens, BLOCK), BF16),
            pltpu.VMEM((tokens, 2 * BLOCK), BF16),
            pltpu.VMEM((blocks, 3 * d, BLOCK), BF16),
            pltpu.VMEM((blocks, 3 * d // 2, BLOCK), BF16),
            pltpu.VMEM((blocks, 3 * d // 2, BLOCK), BF16),
            pltpu.VMEM((blocks, 3 * d // 4, BLOCK), BF16),
            pltpu.VMEM((blocks, 3 * d, BLOCK), BF16),
            pltpu.VMEM((2, BLOCK, d), BF16),
            dma((3,)),
            dma((2, 3)),
        ]
        + [dma((blocks,))] * 14
        + [dma((2, 3))],
        compiler_params=pltpu.CompilerParams(collective_id=0, has_side_effects=True, vmem_limit_bytes=63 * 2**20),
        name="backward",
    )(x, h, dy, *weights)


def adamw(w, m, v, g):
    m = 0.9 * m + 0.1 * g
    v = 0.95 * v + 0.05 * g * g
    step = m * lax.rsqrt(v + 1e-8) + 0.1 * w
    return (w - 0.02 * step).astype(BF16), m, v


def solution(mesh):
    def step(x, dy, *arrays):
        weights, m, v = (arrays[i : i + 3] for i in (0, 3, 6))
        h = forward(x[0], weights)
        *gradients, squares = summed_gradients(x[0], h, dy[0], weights)
        count = sum(g.size for g in gradients)
        factor = jnp.minimum(1.0, 0.5 * lax.rsqrt(jnp.sum(squares) / count + 1e-30))
        new = [adamw(w.astype(F32), m, v, g.astype(F32) * factor) for w, m, v, g in zip(weights, m, v, gradients, strict=True)]
        return tuple(one[which] for which in range(3) for one in new)

    return jax.shard_map(
        step,
        mesh=mesh,
        in_specs=(P(("rep", "dp"), None, None),) * 2 + (P(None, None, None),) * 9,
        out_specs=(P("rep", None, None),) * 9,
        check_vma=False,
    )
```

```python
import functools

import jax
import jax.numpy as jnp
from jax import lax
from jax.experimental import pallas as pl
from jax.experimental.pallas import tpu as pltpu
from jax.sharding import PartitionSpec as P

BLOCK = 256
F32, BF16 = jnp.float32, jnp.bfloat16
TAIL = 3
SUM_LIMIT, OPT_LIMIT = 45 * 2**20, 44 * 2**20
NT = (((1,), (1,)), ((), ()))


def dot(a, b):
    return jnp.dot(a, b, preferred_element_type=F32)


def dot_nt(a, b):
    return lax.dot_general(a, b, NT, preferred_element_type=F32)


def scale_of(wide):
    return lax.rsqrt(jnp.mean(wide * wide, -1, keepdims=True) + 1e-6)


def forward_kernel(tile, chunk, x, wg, wu, wd, out, wgb, wub, wdb, act, sems):
    tokens, ff = x.shape[0], wd.shape[1]
    chunks = ff // chunk

    def copies(f):
        part = pl.ds(pl.multiple_of(f * chunk, chunk), chunk)
        return (
            pltpu.make_async_copy(wg.at[0, :, part], wgb.at[:, part], sems.at[0, f]),
            pltpu.make_async_copy(wu.at[0, :, part], wub.at[:, part], sems.at[1, f]),
            pltpu.make_async_copy(wd.at[0, part, :], wdb.at[part, :], sems.at[2, f]),
        )

    for f in range(chunks):
        for copy in copies(f):
            copy.start()

    def rows_of(t, _):
        rows = pl.ds(pl.multiple_of(t * tile, tile), tile)
        wide = x[rows, :].astype(F32)
        a = (wide * scale_of(wide)).astype(BF16)

        def hidden(f, _):
            @pl.when(t == 0)
            def _():
                for copy in copies(f):
                    copy.wait()

            part = pl.ds(pl.multiple_of(f * chunk, chunk), chunk)
            gate = dot(a, wgb[:, part])
            up = dot(a, wub[:, part])
            act[:, part] = (gate * jax.nn.sigmoid(gate) * up).astype(BF16)
            return 0

        lax.fori_loop(0, chunks, hidden, 0)
        out[rows, :] = x[rows, :] + dot(act[...], wdb[...]).astype(BF16)
        return 0

    lax.fori_loop(0, tokens // tile, rows_of, 0)


def backward_kernel(
    tile, x, h, dy, wg, wu, wd, final, squares,
    hbuf, abuf, at, dbuf, dt, acc, wgu, wdb, act, dgu, grad, pair, edge, middle,
    in_sem, w_sem, p_s, p_r, e_s, e_r, m_s, m_r, f_s, f_r, a_s, a_r, b_s, b_r, q_s, q_r,
):
    tokens, d = abuf.shape
    blocks = wg.shape[2] // BLOCK
    total = 2 * blocks
    ring = grad.shape[0]
    half, quarter = 3 * d // 2, 3 * d // 4
    place = lax.axis_index("dp")
    z, core = place // 2, place % 2
    is_middle = jnp.logical_and(z > 0, z < 3)
    is_edge = jnp.logical_not(is_middle)
    partner = z * 2 + 1 - core
    near = (z + 1 - 2 * (z % 2)) * 2 + core
    across = (3 - z) * 2 + core
    side = z // 2
    own, other = pl.multiple_of(core * half, half), pl.multiple_of((1 - core) * half, half)
    home_in, away_in = pl.multiple_of(side * quarter, quarter), pl.multiple_of((1 - side) * quarter, quarter)
    home, away = pl.multiple_of(own + home_in, quarter), pl.multiple_of(own + away_in, quarter)

    def signal(barrier, device):
        pl.semaphore_signal(barrier, inc=1, device_id={"dp": device}, device_id_type=pl.DeviceIdType.MESH)

    barrier = pltpu.get_barrier_semaphore()
    signal(barrier, partner)
    signal(barrier, near)

    @pl.when(is_middle)
    def _():
        signal(barrier, across)

    pl.semaphore_wait(barrier, jnp.where(is_middle, 3, 2))

    def remote(src, dst, send, recv, device):
        return pltpu.make_async_remote_copy(
            src_ref=src, dst_ref=dst, send_sem=send, recv_sem=recv, device_id={"dp": device}, device_id_type=pl.DeviceIdType.MESH
        )

    def pair_copy(k):
        j = k % ring
        return remote(grad.at[j, pl.ds(other, half), :], pair.at[j], p_s.at[j], p_r.at[j], partner)

    def edge_copy(k, first):
        j, inside, u = k % ring, away_in if first else home_in, 0 if first else 1
        rows = pl.multiple_of(own + inside, quarter)
        return remote(grad.at[j, pl.ds(rows, quarter), :], edge.at[j, pl.ds(inside, quarter), :], e_s.at[j, u], e_r.at[j, u], near)

    def middle_copy(k):
        j = k % ring
        return remote(grad.at[j, pl.ds(away, quarter), :], middle.at[j], m_s.at[j], m_r.at[j], across)

    def hand(k, rows, count, send, recv, device):
        part = final.at[k, pl.ds(rows, count), :]
        return remote(part, part, send, recv, device)

    def cross_copy(k, rows, u=0, parts=1):
        j, count = k % ring, quarter // parts
        return hand(k, pl.multiple_of(rows + u * count, count), count, f_s.at[j, u], f_r.at[j, u], across)

    def back_home(k):
        j = k % ring
        return hand(k, home, quarter, a_s.at[j], a_r.at[j], near)

    def back_away(k, u=0, parts=1):
        j, count = k % ring, quarter // parts
        return hand(k, pl.multiple_of(away + u * count, count), count, b_s.at[j, u], b_r.at[j, u], near)

    def share_home(k, rows):
        j = k % ring
        return hand(k, pl.multiple_of(rows + home_in, quarter), quarter, q_s.at[j, TAIL], q_r.at[j, TAIL], partner)

    def share_away(k, rows, u=0, parts=1):
        j, count = k % ring, quarter // parts
        return hand(k, pl.multiple_of(rows + away_in + u * count, count), count, q_s.at[j, u], q_r.at[j, u], partner)

    def weight_copies(i):
        layer, j, slot = jnp.where(i < blocks, 1, 0), i % blocks, i % 2
        part = pl.ds(pl.multiple_of(j * BLOCK, BLOCK), BLOCK)
        return (
            pltpu.make_async_copy(wg.at[layer, :, part], wgu.at[slot, :, pl.ds(0, BLOCK)], w_sem.at[slot, 0]),
            pltpu.make_async_copy(wu.at[layer, :, part], wgu.at[slot, :, pl.ds(BLOCK, BLOCK)], w_sem.at[slot, 1]),
            pltpu.make_async_copy(wd.at[layer, part, :], wdb.at[slot], w_sem.at[slot, 2]),
        )

    inputs = (
        pltpu.make_async_copy(h, hbuf, in_sem.at[0]),
        pltpu.make_async_copy(dy, dbuf, in_sem.at[1]),
    )
    for copy in weight_copies(0) + inputs:
        copy.start()
    squares[...] = jnp.zeros_like(squares)
    for copy in inputs:
        copy.wait()

    def tiles(body):
        def one(t, _):
            body(pl.ds(pl.multiple_of(t * tile, tile), tile))
            return 0

        lax.fori_loop(0, tokens // tile, one, 0)

    def norm_into(source, rows):
        wide = source[rows, :].astype(F32)
        a = (wide * scale_of(wide)).astype(BF16)
        abuf[rows, :] = a
        at[:, rows] = a.T

    def first(rows):
        norm_into(hbuf, rows)
        dt[:, rows] = dbuf[rows, :].T
        acc[rows, :] = jnp.zeros((tile, d), F32)

    tiles(first)

    def turn(rows):
        wide = hbuf[rows, :].astype(F32)
        by_a = acc[rows, :].astype(BF16).astype(F32)
        r = scale_of(wide)
        by_wide = by_a * r - wide * (r * r * r * jnp.mean(by_a * wide, -1, keepdims=True))
        by_h = by_wide.astype(BF16) + dbuf[rows, :]
        dbuf[rows, :] = by_h
        dt[:, rows] = by_h.T

    def hidden_of(i):
        slot = i % 2
        for copy in weight_copies(i):
            copy.wait()

        @pl.when(i + 1 < total)
        def _():
            for copy in weight_copies(i + 1):
                copy.start()

        @pl.when(i == blocks)
        def _():
            tiles(turn)
            again = pltpu.make_async_copy(x, hbuf, in_sem.at[0])
            again.start()
            again.wait()
            tiles(functools.partial(norm_into, hbuf))

        def hidden(rows):
            gu = dot(abuf[rows, :], wgu[slot])
            by_act = dot_nt(dbuf[rows, :], wdb[slot]).astype(BF16).astype(F32)
            gate, up = gu[:, :BLOCK], gu[:, BLOCK:]
            s = jax.nn.sigmoid(gate)
            silu = gate * s
            act[rows, :] = (silu * up).astype(BF16)
            dgu[rows, :BLOCK] = (by_act * up * (s + silu * (1 - s))).astype(BF16)
            dgu[rows, BLOCK:] = (by_act * silu).astype(BF16)

        tiles(hidden)

    def gradients_of(i):
        j = i % ring
        grad[j, :d, :] = dot(dt[...], act[...]).astype(BF16)
        both = dot(at[...], dgu[...])
        grad[j, d : 2 * d, :] = both[:, :BLOCK].astype(BF16)
        grad[j, 2 * d :, :] = both[:, BLOCK:].astype(BF16)
        pair_copy(i).start()

    def into_of(i):
        slot = i % 2

        def into(rows):
            acc[rows, :] += dot_nt(dgu[rows, :], wgu[slot])

        tiles(into)

    def wide(ref, j, rows, count):
        return ref[j, pl.ds(rows, count), :].astype(F32)

    def paired(k, parts):
        j = k % ring
        pair_copy(k).wait_recv()
        pair_copy(k).wait_send()

        @pl.when(is_edge)
        def _():
            for first, inside, rows in ((True, away_in, away), (False, home_in, home)):
                grad[j, pl.ds(rows, quarter), :] = (wide(grad, j, rows, quarter) + wide(pair, j, inside, quarter)).astype(BF16)
                edge_copy(k, first).start()

    def so_far(j, inside):
        rows = pl.multiple_of(own + inside, quarter)
        return wide(grad, j, rows, quarter) + wide(pair, j, inside, quarter) + wide(edge, j, inside, quarter)

    def sides(k, parts):
        j = k % ring

        @pl.when(is_middle)
        def _():
            edge_copy(k, True).wait_recv()
            grad[j, pl.ds(away, quarter), :] = so_far(j, away_in).astype(BF16)
            middle_copy(k).start()

    def finished(k, parts):
        j, count = k % ring, quarter // parts

        @pl.when(is_middle)
        def _():
            edge_copy(k, False).wait_recv()
            middle_copy(k).wait_recv()
            middle_copy(k).wait_send()
            final[k, pl.ds(home, quarter), :] = (so_far(j, home_in) + wide(middle, j, 0, quarter)).astype(BF16)
            for u in range(parts):
                cross_copy(k, home, u, parts).start()
            back_home(k).start()
            share_home(k, own).start()

    def crossed(k, parts):
        @pl.when(is_middle)
        def _():
            for u in range(parts):
                cross_copy(k, away, u, parts).wait_recv()
                back_away(k, u, parts).start()
                share_away(k, own, u, parts).start()

    def returned(k, parts):
        @pl.when(is_middle)
        def _():
            back_home(k).wait_send()
            for u in range(parts):
                cross_copy(k, home, u, parts).wait_send()
                back_away(k, u, parts).wait_send()

        @pl.when(is_edge)
        def _():
            for first in (True, False):
                edge_copy(k, first).wait_send()
            back_home(k).wait_recv()
            share_home(k, own).start()
            for u in range(parts):
                back_away(k, u, parts).wait_recv()
                share_away(k, own, u, parts).start()

    def shared(k, parts):
        share_home(k, other).wait_recv()
        share_home(k, own).wait_send()
        for u in range(parts):
            share_away(k, other, u, parts).wait_recv()
            share_away(k, own, u, parts).wait_send()
        for part in range(3):
            g = final[k, part * d : (part + 1) * d, :].astype(F32)
            squares[...] += jnp.sum((g * g).reshape(d // 8, 8, BLOCK), axis=0)

    def at_lag(i, lag, stage):
        @pl.when(jnp.logical_and(i >= lag, i < total + lag - 1))
        def _():
            stage(i - lag, 1)

        @pl.when(i == total + lag - 1)
        def _():
            stage(i - lag, TAIL)

    def step(i, _):
        at_lag(i, 6, shared)
        at_lag(i, 5, returned)
        at_lag(i, 3, crossed)

        @pl.when(i < total)
        def _():
            hidden_of(i)

        at_lag(i, 2, finished)

        @pl.when(i < total)
        def _():
            gradients_of(i)

        at_lag(i, 1, sides)

        @pl.when(i < blocks)
        def _():
            into_of(i)

        at_lag(i, 0, paired)
        return 0

    lax.fori_loop(0, total + 6, step, 0)


def optimizer_kernel(depth, g, squares, *refs):
    w, m, v, new_w, new_m, new_v = (refs[i : i + 3] for i in range(0, 18, 3))
    in_bufs, out_bufs, turned, in_sem, out_sem = refs[18:27], refs[27:36], refs[36], refs[37], refs[38]
    blocks = w[0].shape[2] // BLOCK
    total = 2 * blocks
    d = w[0].shape[1]
    count = 3 * 2 * d * w[0].shape[2]
    factor = jnp.minimum(1.0, 0.5 * lax.rsqrt(jnp.sum(squares[...], keepdims=True) / count + 1e-30))

    def views(arrays, k):
        layer, part = jnp.where(k < blocks, 1, 0), pl.ds(pl.multiple_of((k % blocks) * BLOCK, BLOCK), BLOCK)
        return [a.at[layer, part, :] if i % 3 == 2 else a.at[layer, :, part] for i, a in enumerate(arrays)]

    def ins(k):
        slot = k % depth
        return [pltpu.make_async_copy(a, b.at[slot], in_sem.at[slot, i]) for i, (a, b) in enumerate(zip(views(w + m + v, k), in_bufs, strict=True))]

    def outs(k):
        slot = k % 2
        return [
            pltpu.make_async_copy(b.at[slot], a, out_sem.at[slot, i])
            for i, (a, b) in enumerate(zip(views(new_w + new_m + new_v, k), out_bufs, strict=True))
        ]

    for k in range(depth - 1):
        for copy in ins(k):
            copy.start()

    def step(k, _):
        slot, out_slot = k % depth, k % 2

        @pl.when(k + depth - 1 < total)
        def _():
            for copy in ins(k + depth - 1):
                copy.start()

        @pl.when(k >= 2)
        def _():
            for copy in outs(k - 2):
                copy.wait()

        for copy in ins(k):
            copy.wait()
        turned[...] = g[k, :d, :].T
        for i in range(3):
            rows_in_all = BLOCK if i == 2 else d
            rows_at_once = 32

            def part(r, _, i=i, rows_at_once=rows_at_once):
                rows = pl.ds(pl.multiple_of(r * rows_at_once, rows_at_once), rows_at_once)
                raw = turned[rows, :] if i == 2 else g[k, pl.ds(pl.multiple_of((i + 1) * d + r * rows_at_once, rows_at_once), rows_at_once), :]
                one = raw.astype(F32) * factor
                old = in_bufs[i][slot, rows, :].astype(F32)
                first = 0.9 * in_bufs[3 + i][slot, rows, :] + 0.1 * one
                second = 0.95 * in_bufs[6 + i][slot, rows, :] + 0.05 * one * one
                out_bufs[i][out_slot, rows, :] = (old - 0.02 * (first * lax.rsqrt(second + 1e-8) + 0.1 * old)).astype(BF16)
                out_bufs[3 + i][out_slot, rows, :] = first
                out_bufs[6 + i][out_slot, rows, :] = second
                return 0

            lax.fori_loop(0, rows_in_all // rows_at_once, part, 0)
        for copy in outs(k):
            copy.start()
        return 0

    lax.fori_loop(0, total, step, 0)
    for k in (total - 2, total - 1):
        for copy in outs(k):
            copy.wait()


def forward(x, weights, tile=512, chunk=512):
    tokens, d = x.shape
    ff = weights[0].shape[2]
    any_space = pl.BlockSpec(memory_space=pl.ANY)
    return pl.pallas_call(
        functools.partial(forward_kernel, min(tile, tokens), chunk),
        out_shape=jax.ShapeDtypeStruct(x.shape, BF16),
        in_specs=[pl.BlockSpec(memory_space=pltpu.VMEM)] + [any_space] * 3,
        out_specs=pl.BlockSpec(memory_space=pltpu.VMEM),
        scratch_shapes=[
            pltpu.VMEM((d, ff), BF16),
            pltpu.VMEM((d, ff), BF16),
            pltpu.VMEM((ff, d), BF16),
            pltpu.VMEM((min(tile, tokens), ff), BF16),
            pltpu.SemaphoreType.DMA((3, ff // chunk)),
        ],
        compiler_params=pltpu.CompilerParams(vmem_limit_bytes=48 * 2**20),
        name="forward",
    )(x, *weights)


def summed_gradients(x, h, dy, weights, tile=512, ring=8):
    tokens, d = x.shape
    blocks = weights[0].shape[2] // BLOCK
    tile = min(tile, tokens)
    any_space = pl.BlockSpec(memory_space=pl.ANY)
    vmem = pl.BlockSpec(memory_space=pltpu.VMEM)
    dma = pltpu.SemaphoreType.DMA
    return pl.pallas_call(
        functools.partial(backward_kernel, tile),
        out_shape=[pltpu.VMEM((2 * blocks, 3 * d, BLOCK), BF16), jax.ShapeDtypeStruct((8, BLOCK), F32)],
        in_specs=[any_space] * 6,
        out_specs=[vmem, vmem],
        scratch_shapes=[
            pltpu.VMEM((tokens, d), BF16),
            pltpu.VMEM((tokens, d), BF16),
            pltpu.VMEM((d, tokens), BF16),
            pltpu.VMEM((tokens, d), BF16),
            pltpu.VMEM((d, tokens), BF16),
            pltpu.VMEM((tokens, d), F32),
            pltpu.VMEM((2, d, 2 * BLOCK), BF16),
            pltpu.VMEM((2, BLOCK, d), BF16),
            pltpu.VMEM((tokens, BLOCK), BF16),
            pltpu.VMEM((tokens, 2 * BLOCK), BF16),
            pltpu.VMEM((ring, 3 * d, BLOCK), BF16),
            pltpu.VMEM((ring, 3 * d // 2, BLOCK), BF16),
            pltpu.VMEM((ring, 3 * d // 2, BLOCK), BF16),
            pltpu.VMEM((ring, 3 * d // 4, BLOCK), BF16),
            dma((2,)),
            dma((2, 3)),
        ]
        + [dma(size) for size in ((ring,), (ring, 2), (ring,), (ring, TAIL), (ring,), (ring, TAIL), (ring, TAIL + 1)) for _ in range(2)],
        compiler_params=pltpu.CompilerParams(collective_id=0, has_side_effects=True, vmem_limit_bytes=SUM_LIMIT),
        name="backward",
    )(x, h, dy, *weights)


def optimizer(g, squares, w, m, v, depth=3):
    d, ff = w[0].shape[1:]
    any_space = pl.BlockSpec(memory_space=pl.ANY)
    vmem = pl.BlockSpec(memory_space=pltpu.VMEM)
    shapes = [(d, BLOCK), (d, BLOCK), (BLOCK, d)] * 3
    dtypes = [BF16] * 3 + [F32] * 6
    return pl.pallas_call(
        functools.partial(optimizer_kernel, depth),
        out_shape=[jax.ShapeDtypeStruct(a.shape, a.dtype) for a in (*w, *m, *v)],
        in_specs=[vmem] * 2 + [any_space] * 9,
        out_specs=[any_space] * 9,
        scratch_shapes=[pltpu.VMEM((depth, *s), t) for s, t in zip(shapes, dtypes, strict=True)]
        + [pltpu.VMEM((2, *s), t) for s, t in zip(shapes, dtypes, strict=True)]
        + [pltpu.VMEM((BLOCK, d), BF16), pltpu.SemaphoreType.DMA((depth, 9)), pltpu.SemaphoreType.DMA((2, 9))],
        compiler_params=pltpu.CompilerParams(vmem_limit_bytes=OPT_LIMIT),
        name="optimizer",
    )(pltpu.with_memory_space_constraint(g, pltpu.VMEM), squares, *w, *m, *v)


def solution(mesh):
    def step(x, dy, *arrays):
        weights, m, v = (arrays[i : i + 3] for i in (0, 3, 6))
        h = forward(x[0], weights)
        g, squares = summed_gradients(x[0], h, dy[0], weights)
        return tuple(optimizer(g, squares, weights, m, v))

    return jax.shard_map(
        step,
        mesh=mesh,
        in_specs=(P(("rep", "dp"), None, None),) * 2 + (P(None, None, None),) * 9,
        out_specs=(P("rep", None, None),) * 9,
        check_vma=False,
    )
```

```python
import functools

import jax
import jax.numpy as jnp
from jax import lax
from jax.experimental import pallas as pl
from jax.experimental.pallas import tpu as pltpu
from jax.sharding import PartitionSpec as P

BLOCK = 256
F32, BF16 = jnp.float32, jnp.bfloat16
TAIL = 3
FORWARD_LIMIT, SUM_LIMIT, OPT_LIMIT = int(61.4 * 2**20), 40 * 2**20, 40 * 2**20
NT = (((1,), (1,)), ((), ()))


def dot(a, b):
    return jnp.dot(a, b, preferred_element_type=F32)


def dot_nt(a, b):
    return lax.dot_general(a, b, NT, preferred_element_type=F32)


def scale_of(wide):
    return lax.rsqrt(jnp.mean(wide * wide, -1, keepdims=True) + 1e-6)


def forward_kernel(tile, chunk, source, wg, wu, wd, out, x, wgb, wub, wdb, act, sems, x_sem, down_sem):
    tokens, ff = x.shape[0], wd.shape[1]
    chunks = ff // chunk

    def copies(f):
        part = pl.ds(pl.multiple_of(f * chunk, chunk), chunk)
        return (
            pltpu.make_async_copy(wg.at[0, :, part], wgb.at[:, part], sems.at[0, f]),
            pltpu.make_async_copy(wu.at[0, :, part], wub.at[:, part], sems.at[1, f]),
        )

    down_copy = pltpu.make_async_copy(wd.at[0], wdb, down_sem)

    def x_copy(t):
        rows = pl.ds(pl.multiple_of(t * tile, tile), tile)
        return pltpu.make_async_copy(source.at[rows, :], x.at[rows, :], x_sem.at[t])

    x_copy(0).start()
    for f in range(chunks):
        for copy in copies(f):
            copy.start()
    down_copy.start()
    for t in range(1, tokens // tile):
        x_copy(t).start()

    def rows_of(t, _):
        x_copy(t).wait()
        rows = pl.ds(pl.multiple_of(t * tile, tile), tile)
        wide = x[rows, :].astype(F32)
        a = (wide * scale_of(wide)).astype(BF16)

        def hidden(f, _):
            @pl.when(t == 0)
            def _():
                for copy in copies(f):
                    copy.wait()

            part = pl.ds(pl.multiple_of(f * chunk, chunk), chunk)
            gate = dot(a, wgb[:, part])
            up = dot(a, wub[:, part])
            act[:, part] = (gate * jax.nn.sigmoid(gate) * up).astype(BF16)
            return 0

        lax.fori_loop(0, chunks, hidden, 0)

        @pl.when(t == 0)
        def _():
            down_copy.wait()

        out[rows, :] = x[rows, :] + dot(act[...], wdb[...]).astype(BF16)
        return 0

    lax.fori_loop(0, tokens // tile, rows_of, 0)


def block_views(arrays, k, blocks):
    layer, part = jnp.where(k < blocks, 1, 0), pl.ds(pl.multiple_of((k % blocks) * BLOCK, BLOCK), BLOCK)
    return [a.at[layer, part, :] if i % 3 == 2 else a.at[layer, :, part] for i, a in enumerate(arrays)]


def backward_kernel(
    tile, x, h, dy, wg, wu, wd, final, squares,
    abuf, at, dbuf, dt, acc, wgu, wdb, act, dgu, grad, pair, edge, middle,
    in_sem, w_sem, p_s, p_r, e_s, e_r, m_s, m_r, f_s, f_r, a_s, a_r, b_s, b_r, q_s, q_r,
):
    tokens, d = abuf.shape
    blocks = wg.shape[2] // BLOCK
    total = 2 * blocks
    ring = grad.shape[0]
    half, quarter = 3 * d // 2, 3 * d // 4
    place = lax.axis_index("dp")
    z, core = place // 2, place % 2
    is_middle = jnp.logical_and(z > 0, z < 3)
    is_edge = jnp.logical_not(is_middle)
    partner = z * 2 + 1 - core
    near = (z + 1 - 2 * (z % 2)) * 2 + core
    across = (3 - z) * 2 + core
    side = z // 2
    own, other = pl.multiple_of(core * half, half), pl.multiple_of((1 - core) * half, half)
    home_in, away_in = pl.multiple_of(side * quarter, quarter), pl.multiple_of((1 - side) * quarter, quarter)
    home, away = pl.multiple_of(own + home_in, quarter), pl.multiple_of(own + away_in, quarter)

    def signal(barrier, device):
        pl.semaphore_signal(barrier, inc=1, device_id={"dp": device}, device_id_type=pl.DeviceIdType.MESH)

    barrier = pltpu.get_barrier_semaphore()
    signal(barrier, partner)
    signal(barrier, near)

    @pl.when(is_middle)
    def _():
        signal(barrier, across)

    pl.semaphore_wait(barrier, jnp.where(is_middle, 3, 2))

    def remote(src, dst, send, recv, device):
        return pltpu.make_async_remote_copy(
            src_ref=src, dst_ref=dst, send_sem=send, recv_sem=recv, device_id={"dp": device}, device_id_type=pl.DeviceIdType.MESH
        )

    def pair_copy(k):
        j = k % ring
        return remote(grad.at[j, pl.ds(other, half), :], pair.at[j], p_s.at[j], p_r.at[j], partner)

    def edge_copy(k, first):
        j, inside, u = k % ring, away_in if first else home_in, 0 if first else 1
        rows = pl.multiple_of(own + inside, quarter)
        return remote(grad.at[j, pl.ds(rows, quarter), :], edge.at[j, pl.ds(inside, quarter), :], e_s.at[j, u], e_r.at[j, u], near)

    def middle_copy(k):
        j = k % ring
        return remote(grad.at[j, pl.ds(away, quarter), :], middle.at[j], m_s.at[j], m_r.at[j], across)

    def hand(k, rows, count, send, recv, device):
        part = final.at[k, pl.ds(rows, count), :]
        return remote(part, part, send, recv, device)

    def cross_copy(k, rows, u=0, parts=1):
        j, count = k % ring, quarter // parts
        return hand(k, pl.multiple_of(rows + u * count, count), count, f_s.at[j, u], f_r.at[j, u], across)

    def back_home(k):
        j = k % ring
        return hand(k, home, quarter, a_s.at[j], a_r.at[j], near)

    def back_away(k, u=0, parts=1):
        j, count = k % ring, quarter // parts
        return hand(k, pl.multiple_of(away + u * count, count), count, b_s.at[j, u], b_r.at[j, u], near)

    def share_home(k, rows):
        j = k % ring
        return hand(k, pl.multiple_of(rows + home_in, quarter), quarter, q_s.at[j, TAIL], q_r.at[j, TAIL], partner)

    def share_away(k, rows, u=0, parts=1):
        j, count = k % ring, quarter // parts
        return hand(k, pl.multiple_of(rows + away_in + u * count, count), count, q_s.at[j, u], q_r.at[j, u], partner)

    def weight_copies(i):
        layer, j, slot = jnp.where(i < blocks, 1, 0), i % blocks, i % 2
        part = pl.ds(pl.multiple_of(j * BLOCK, BLOCK), BLOCK)
        return (
            pltpu.make_async_copy(wg.at[layer, :, part], wgu.at[slot, :, pl.ds(0, BLOCK)], w_sem.at[slot, 0]),
            pltpu.make_async_copy(wu.at[layer, :, part], wgu.at[slot, :, pl.ds(BLOCK, BLOCK)], w_sem.at[slot, 1]),
            pltpu.make_async_copy(wd.at[layer, part, :], wdb.at[slot], w_sem.at[slot, 2]),
        )

    given = pltpu.make_async_copy(dy, dbuf, in_sem.at[0])
    given.start()
    for copy in weight_copies(0):
        copy.start()
    squares[...] = jnp.zeros_like(squares)
    given.wait()

    def tiles(body):
        def one(t, _):
            body(pl.ds(pl.multiple_of(t * tile, tile), tile))
            return 0

        lax.fori_loop(0, tokens // tile, one, 0)

    def norm_into(source, rows):
        wide = source[rows, :].astype(F32)
        a = (wide * scale_of(wide)).astype(BF16)
        abuf[rows, :] = a
        at[:, rows] = a.T

    def first(rows):
        norm_into(h, rows)
        dt[:, rows] = dbuf[rows, :].T
        acc[rows, :] = jnp.zeros((tile, d), F32)

    tiles(first)

    def turn(rows):
        wide = h[rows, :].astype(F32)
        by_a = acc[rows, :].astype(BF16).astype(F32)
        r = scale_of(wide)
        by_wide = by_a * r - wide * (r * r * r * jnp.mean(by_a * wide, -1, keepdims=True))
        by_h = by_wide.astype(BF16) + dbuf[rows, :]
        dbuf[rows, :] = by_h
        dt[:, rows] = by_h.T

    def hidden_of(i):
        slot = i % 2
        for copy in weight_copies(i):
            copy.wait()

        @pl.when(i + 1 < total)
        def _():
            for copy in weight_copies(i + 1):
                copy.start()

        @pl.when(i == blocks)
        def _():
            again = pltpu.make_async_copy(x, abuf, in_sem.at[1])
            again.start()
            tiles(turn)
            again.wait()
            tiles(functools.partial(norm_into, abuf))

        def hidden(rows):
            gu = dot(abuf[rows, :], wgu[slot])
            by_act = dot_nt(dbuf[rows, :], wdb[slot]).astype(BF16).astype(F32)
            gate, up = gu[:, :BLOCK], gu[:, BLOCK:]
            s = jax.nn.sigmoid(gate)
            silu = gate * s
            act[rows, :] = (silu * up).astype(BF16)
            dgu[rows, :BLOCK] = (by_act * up * (s + silu * (1 - s))).astype(BF16)
            dgu[rows, BLOCK:] = (by_act * silu).astype(BF16)

        tiles(hidden)

    def gradients_of(i):
        j = i % ring
        grad[j, :d, :] = dot(dt[...], act[...]).astype(BF16)
        both = dot(at[...], dgu[...])
        grad[j, d : 2 * d, :] = both[:, :BLOCK].astype(BF16)
        grad[j, 2 * d :, :] = both[:, BLOCK:].astype(BF16)
        pair_copy(i).start()

    def into_of(i):
        slot = i % 2

        def into(rows):
            acc[rows, :] += dot_nt(dgu[rows, :], wgu[slot])

        tiles(into)

    def wide(ref, j, rows, count):
        return ref[j, pl.ds(rows, count), :].astype(F32)

    def paired(k, parts):
        j = k % ring
        pair_copy(k).wait_recv()
        pair_copy(k).wait_send()

        @pl.when(is_edge)
        def _():
            for first, inside, rows in ((True, away_in, away), (False, home_in, home)):
                grad[j, pl.ds(rows, quarter), :] = (wide(grad, j, rows, quarter) + wide(pair, j, inside, quarter)).astype(BF16)
                edge_copy(k, first).start()

    def so_far(j, inside):
        rows = pl.multiple_of(own + inside, quarter)
        return wide(grad, j, rows, quarter) + wide(pair, j, inside, quarter) + wide(edge, j, inside, quarter)

    def sides(k, parts):
        j = k % ring

        @pl.when(is_middle)
        def _():
            edge_copy(k, True).wait_recv()
            grad[j, pl.ds(away, quarter), :] = so_far(j, away_in).astype(BF16)
            middle_copy(k).start()

    def finished(k, parts):
        j, count = k % ring, quarter // parts

        @pl.when(is_middle)
        def _():
            edge_copy(k, False).wait_recv()
            middle_copy(k).wait_recv()
            middle_copy(k).wait_send()
            final[k, pl.ds(home, quarter), :] = (so_far(j, home_in) + wide(middle, j, 0, quarter)).astype(BF16)
            for u in range(parts):
                cross_copy(k, home, u, parts).start()
            back_home(k).start()
            share_home(k, own).start()

    def crossed(k, parts):
        @pl.when(is_middle)
        def _():
            for u in range(parts):
                cross_copy(k, away, u, parts).wait_recv()
                back_away(k, u, parts).start()
                share_away(k, own, u, parts).start()

    def returned(k, parts):
        @pl.when(is_middle)
        def _():
            back_home(k).wait_send()
            for u in range(parts):
                cross_copy(k, home, u, parts).wait_send()
                back_away(k, u, parts).wait_send()

        @pl.when(is_edge)
        def _():
            for first in (True, False):
                edge_copy(k, first).wait_send()
            back_home(k).wait_recv()
            share_home(k, own).start()
            for u in range(parts):
                back_away(k, u, parts).wait_recv()
                share_away(k, own, u, parts).start()

    def shared(k, parts):
        share_home(k, other).wait_recv()
        share_home(k, own).wait_send()
        for u in range(parts):
            share_away(k, other, u, parts).wait_recv()
            share_away(k, own, u, parts).wait_send()
        for part in range(3):
            g = final[k, part * d : (part + 1) * d, :].astype(F32)
            squares[...] += jnp.sum((g * g).reshape(d // 8, 8, BLOCK), axis=0)

    def at_lag(i, lag, stage):
        @pl.when(jnp.logical_and(i >= lag, i < total + lag - 1))
        def _():
            stage(i - lag, 1)

        @pl.when(i == total + lag - 1)
        def _():
            stage(i - lag, TAIL)

    def step(i, _):
        at_lag(i, 6, shared)
        at_lag(i, 5, returned)
        at_lag(i, 3, crossed)

        @pl.when(i < total)
        def _():
            hidden_of(i)

        at_lag(i, 2, finished)

        @pl.when(i < total)
        def _():
            gradients_of(i)

        at_lag(i, 1, sides)

        @pl.when(i < blocks)
        def _():
            into_of(i)

        at_lag(i, 0, paired)
        return 0

    lax.fori_loop(0, total + 6, step, 0)


def optimizer_kernel(depth, g, squares, *refs):
    w, m, v, new_w, new_m, new_v = (refs[i : i + 3] for i in range(0, 18, 3))
    in_bufs, out_bufs, turned, in_sem, out_sem = refs[18:27], refs[27:36], refs[36], refs[37], refs[38]
    blocks = w[0].shape[2] // BLOCK
    total = 2 * blocks
    d = w[0].shape[1]
    count = 3 * 2 * d * w[0].shape[2]
    factor = jnp.minimum(1.0, 0.5 * lax.rsqrt(jnp.sum(squares[...], keepdims=True) / count + 1e-30))

    def ins(k):
        slot = k % depth
        return [pltpu.make_async_copy(a, b.at[slot], in_sem.at[slot, i]) for i, (a, b) in enumerate(zip(block_views(w + m + v, k, blocks), in_bufs, strict=True))]

    def outs(k):
        slot = k % 2
        return [
            pltpu.make_async_copy(b.at[slot], a, out_sem.at[slot, i])
            for i, (a, b) in enumerate(zip(block_views(new_w + new_m + new_v, k, blocks), out_bufs, strict=True))
        ]

    for k in range(depth - 1):
        for copy in ins(k):
            copy.start()

    def update(k, old_refs):
        out_slot = k % 2
        turned[...] = g[k, :d, :].T
        for i in range(3):
            rows_in_all = BLOCK if i == 2 else d
            rows_at_once = 32

            def part(r, _, i=i, rows_at_once=rows_at_once):
                rows = pl.ds(pl.multiple_of(r * rows_at_once, rows_at_once), rows_at_once)
                raw = turned[rows, :] if i == 2 else g[k, pl.ds(pl.multiple_of((i + 1) * d + r * rows_at_once, rows_at_once), rows_at_once), :]
                one = raw.astype(F32) * factor
                old = old_refs[i][rows, :].astype(F32)
                first = 0.9 * old_refs[3 + i][rows, :] + 0.1 * one
                second = 0.95 * old_refs[6 + i][rows, :] + 0.05 * one * one
                out_bufs[i][out_slot, rows, :] = (old - 0.02 * (first * lax.rsqrt(second + 1e-8) + 0.1 * old)).astype(BF16)
                out_bufs[3 + i][out_slot, rows, :] = first
                out_bufs[6 + i][out_slot, rows, :] = second
                return 0

            lax.fori_loop(0, rows_in_all // rows_at_once, part, 0)
        for copy in outs(k):
            copy.start()

    def step(k, _):
        @pl.when(k + depth - 1 < total)
        def _():
            for copy in ins(k + depth - 1):
                copy.start()

        @pl.when(k >= 2)
        def _():
            for copy in outs(k - 2):
                copy.wait()

        for copy in ins(k):
            copy.wait()
        update(k, [b.at[k % depth] for b in in_bufs])
        return 0

    lax.fori_loop(0, total, step, 0)
    for k in (total - 2, total - 1):
        for copy in outs(k):
            copy.wait()


def pinned(a):
    return pltpu.with_memory_space_constraint(a, pltpu.VMEM)


def block_shapes(d):
    return list(zip([(d, BLOCK), (d, BLOCK), (BLOCK, d)] * 3, [BF16] * 3 + [F32] * 6, strict=True))


def forward(x, weights, tile=1024, chunk=512):
    tokens, d = x.shape
    ff = weights[0].shape[2]
    any_space = pl.BlockSpec(memory_space=pltpu.HBM)
    return pl.pallas_call(
        functools.partial(forward_kernel, min(tile, tokens), chunk),
        out_shape=pltpu.VMEM(x.shape, BF16),
        in_specs=[any_space] * 4,
        out_specs=pl.BlockSpec(memory_space=pltpu.VMEM),
        scratch_shapes=[
            pltpu.VMEM((tokens, d), BF16),
            pltpu.VMEM((d, ff), BF16),
            pltpu.VMEM((d, ff), BF16),
            pltpu.VMEM((ff, d), BF16),
            pltpu.VMEM((min(tile, tokens), ff), BF16),
            pltpu.SemaphoreType.DMA((2, ff // chunk)),
            pltpu.SemaphoreType.DMA((tokens // min(tile, tokens),)),
            pltpu.SemaphoreType.DMA(()),
        ],
        compiler_params=pltpu.CompilerParams(vmem_limit_bytes=FORWARD_LIMIT),
        name="forward",
    )(x, *weights)


def summed_gradients(x, h, dy, w, tile=1024, ring=7):
    tokens, d = x.shape
    blocks = w[0].shape[2] // BLOCK
    tile = min(tile, tokens)
    any_space = pl.BlockSpec(memory_space=pltpu.HBM)
    vmem = pl.BlockSpec(memory_space=pltpu.VMEM)
    dma = pltpu.SemaphoreType.DMA
    return pl.pallas_call(
        functools.partial(backward_kernel, tile),
        out_shape=[pltpu.VMEM((2 * blocks, 3 * d, BLOCK), BF16), jax.ShapeDtypeStruct((8, BLOCK), F32)],
        in_specs=[any_space, vmem] + [any_space] * 4,
        out_specs=[vmem] * 2,
        scratch_shapes=[
            pltpu.VMEM((tokens, d), BF16),
            pltpu.VMEM((d, tokens), BF16),
            pltpu.VMEM((tokens, d), BF16),
            pltpu.VMEM((d, tokens), BF16),
            pltpu.VMEM((tokens, d), F32),
            pltpu.VMEM((2, d, 2 * BLOCK), BF16),
            pltpu.VMEM((2, BLOCK, d), BF16),
            pltpu.VMEM((tokens, BLOCK), BF16),
            pltpu.VMEM((tokens, 2 * BLOCK), BF16),
            pltpu.VMEM((ring, 3 * d, BLOCK), BF16),
            pltpu.VMEM((ring, 3 * d // 2, BLOCK), BF16),
            pltpu.VMEM((ring, 3 * d // 2, BLOCK), BF16),
            pltpu.VMEM((ring, 3 * d // 4, BLOCK), BF16),
            dma((2,)),
            dma((2, 3)),
        ]
        + [dma(size) for size in ((ring,), (ring, 2), (ring,), (ring, TAIL), (ring,), (ring, TAIL), (ring, TAIL + 1)) for _ in range(2)],
        compiler_params=pltpu.CompilerParams(collective_id=0, has_side_effects=True, vmem_limit_bytes=SUM_LIMIT),
        name="backward",
    )(x, pinned(h), dy, *w)


def optimizer(g, squares, w, m, v, depth=4):
    d = w[0].shape[1]
    any_space = pl.BlockSpec(memory_space=pltpu.HBM)
    vmem = pl.BlockSpec(memory_space=pltpu.VMEM)
    blocks = block_shapes(d)
    return pl.pallas_call(
        functools.partial(optimizer_kernel, depth),
        out_shape=[jax.ShapeDtypeStruct(a.shape, a.dtype) for a in (*w, *m, *v)],
        in_specs=[vmem] * 2 + [any_space] * 9,
        out_specs=[any_space] * 9,
        scratch_shapes=[pltpu.VMEM((depth, *s), t) for s, t in blocks]
        + [pltpu.VMEM((2, *s), t) for s, t in blocks]
        + [pltpu.VMEM((BLOCK, d), BF16), pltpu.SemaphoreType.DMA((depth, 9)), pltpu.SemaphoreType.DMA((2, 9))],
        compiler_params=pltpu.CompilerParams(vmem_limit_bytes=OPT_LIMIT),
        name="optimizer",
    )(pinned(g), squares, *w, *m, *v)


def solution(mesh):
    def step(x, dy, *arrays):
        weights, m, v = (arrays[i : i + 3] for i in (0, 3, 6))
        h = forward(x[0], weights)
        g, squares = summed_gradients(x[0], h, dy[0], weights)
        return tuple(optimizer(g, squares, weights, m, v))

    return jax.shard_map(
        step,
        mesh=mesh,
        in_specs=(P(("rep", "dp"), None, None),) * 2 + (P(None, None, None),) * 9,
        out_specs=(P("rep", None, None),) * 9,
        check_vma=False,
    )
```
